32 devices in a mesh: zero: 8 (over z, x), model: 4 (over y, core).
Axes of the slice: x: 2, y: 2, z: 4, core: 2. Of those that a mesh axis runs over, the one named last changes fastest.
Arguments:
- w_query: bfloat16 [4096, 4096], P('zero', 'model'), may hold values from -0.125 to 0.125
- low_query: bfloat16 [4096, 16], P('zero'), may hold values from -0.09375 to 0.09375
- high_query: bfloat16 [16, 4096], P(None, 'model'), may hold values from -1.5 to 1.5
- w_key: bfloat16 [4096, 4096], P('zero', 'model'), may hold values from -0.125 to 0.125
- low_key: bfloat16 [4096, 16], P('zero'), may hold values from -0.09375 to 0.09375
- high_key: bfloat16 [16, 4096], P(None, 'model'), may hold values from -1.5 to 1.5
- w_value: bfloat16 [4096, 4096], P('zero', 'model'), may hold values from -0.125 to 0.125
- low_value: bfloat16 [4096, 16], P('zero'), may hold values from -0.09375 to 0.09375
- high_value: bfloat16 [16, 4096], P(None, 'model'), may hold values from -1.5 to 1.5
- norm_train: float32 [4096], P(('zero', 'model')), may hold values from 0.25 to 1.75
- norm_step: float32 [4096], P(('zero', 'model')), may hold values from -0.3 to 0.3
Outputs:
- serving_query: bfloat16 [4096, 4096], P(None, 'model')
- serving_key: bfloat16 [4096, 4096], P(None, 'model')
- serving_value: bfloat16 [4096, 4096], P(None, 'model')
- factor_query: float32 [4096], P('model')
- factor_key: float32 [4096], P('model')
- factor_value: float32 [4096], P('model')
- serve_norm: bfloat16 [4096], replicated
The draws below stay inside these ranges and needn't reach their ends.
All inputs are finite; a program needn't handle non-finite values. Where the reference program divides by a largest or mean magnitude, that divisor is 1e-20 or more.
Results may differ from the reference program's by a relative error of at most 0.001.
Values may be sent and summed in bfloat16 or wider, within the bound.
A program may use at most 128 MiB of HBM per device.

```python
import jax
import jax.numpy as jnp

D_MODEL = 4096
Q_DIM = 4096
KV_DIM = 4096
RANK = 16


def spiked(array, stream_key, source, target, parts, factor):
    def block_of(axis_at):
        return (jnp.arange(array.shape[axis_at]) // (array.shape[axis_at] // parts)).reshape((-1,) + (1,) * (array.ndim - 1 - axis_at))

    first = jax.random.permutation(stream_key, parts)[block_of(target)]
    other_side = (block_of(target) + parts // 2) % parts
    return jnp.where((block_of(source) == first) | (block_of(source) == other_side), factor * array, array)


def block_levels(key, dims, cuts, least, largest):
    loudness = 1.0
    for axis_at, parts in cuts:
        heights = jax.random.uniform(jax.random.fold_in(jax.random.fold_in(key, 6), axis_at), (parts,), jnp.float32, least / len(cuts), largest / len(cuts))
        loudness = loudness * jnp.repeat(jnp.exp(heights), dims[axis_at] // parts).reshape((-1,) + (1,) * (len(dims) - 1 - axis_at))
    return loudness


def noise(own_key, extent, width, bound, cuts=(), kind=jnp.bfloat16):
    array = width * jax.random.normal(own_key, extent, jnp.float32)
    if cuts:
        array = array * block_levels(own_key, extent, cuts, -0.22, 0.18)
    return jnp.clip(array, -bound, bound).astype(kind)


def bell_draw_with(rng, extent, scale, reach, pieces, heavy, held_as=jnp.bfloat16):
    drawn = scale * jax.random.normal(rng, extent, jnp.float32)
    if pieces:
        drawn = drawn * block_levels(rng, extent, pieces, -0.22, 0.18)
    return jnp.clip(spiked(drawn, jax.random.fold_in(rng, 3), *heavy), -reach, reach).astype(held_as)


def setup_inputs(seed: int = 0) -> dict:
    key_list = jax.random.split(jax.random.key(seed), 12)
    return {
        "w_query": bell_draw_with(key_list[0], (D_MODEL, Q_DIM), D_MODEL ** -0.5, 0.125, ((0, 8), (1, 4)), (0, 1, 8, 2.0)),
        "low_query": noise(key_list[1], (D_MODEL, RANK), D_MODEL ** -0.5, 0.09375, ((0, 8),)),
        "high_query": noise(key_list[2], (RANK, Q_DIM), RANK ** -0.5, 1.5, ((1, 4),)),
        "w_key": bell_draw_with(key_list[3], (D_MODEL, KV_DIM), D_MODEL ** -0.5, 0.125, ((0, 8), (1, 4)), (0, 1, 8, 2.0)),
        "low_key": noise(key_list[4], (D_MODEL, RANK), D_MODEL ** -0.5, 0.09375, ((0, 8),)),
        "high_key": noise(key_list[5], (RANK, KV_DIM), RANK ** -0.5, 1.5, ((1, 4),)),
        "w_value": bell_draw_with(key_list[6], (D_MODEL, KV_DIM), D_MODEL ** -0.5, 0.125, ((0, 8), (1, 4)), (0, 1, 8, 2.0)),
        "low_value": noise(key_list[7], (D_MODEL, RANK), D_MODEL ** -0.5, 0.09375, ((0, 8),)),
        "high_value": noise(key_list[8], (RANK, KV_DIM), RANK ** -0.5, 1.5, ((1, 4),)),
        "norm_train": jnp.clip(1.0 + 0.15 * jax.random.normal(key_list[9], (D_MODEL,), jnp.float32), 0.25, 1.75),
        "norm_step": jnp.clip(jax.random.uniform(key_list[10], (D_MODEL,), jnp.float32, -0.3, 0.3) * block_levels(key_list[10], (D_MODEL,), ((0, 32),), -0.4, 0.0), -0.3, 0.3),
    }


mix_rate = 0.5


def reference(w_query, low_query, high_query, w_key, low_key, high_key, w_value, low_value, high_value, norm_train, norm_step):
    whole_query = w_query.astype(jnp.float32) + mix_rate * jnp.dot(low_query, high_query, preferred_element_type=jnp.float32)
    whole_key = w_key.astype(jnp.float32) + mix_rate * jnp.dot(low_key, high_key, preferred_element_type=jnp.float32)
    whole_value = w_value.astype(jnp.float32) + mix_rate * jnp.dot(low_value, high_value, preferred_element_type=jnp.float32)
    factor_query = jnp.sum(jnp.abs(whole_query), axis=0) / D_MODEL
    serving_query = (whole_query / factor_query).astype(jnp.bfloat16)
    factor_key = jnp.sum(jnp.abs(whole_key), axis=0) / D_MODEL
    serving_key = (whole_key / factor_key).astype(jnp.bfloat16)
    factor_value = jnp.sum(jnp.abs(whole_value), axis=0) / D_MODEL
    serving_value = (whole_value / factor_value).astype(jnp.bfloat16)
    serve_norm = (norm_train + norm_step).astype(jnp.bfloat16)
    return serving_query, serving_key, serving_value, factor_query, factor_key, factor_value, serve_norm
```

```python
import functools

import jax
import jax.numpy as jnp
from jax import lax
from jax.experimental import pallas as pl
from jax.experimental.pallas import tpu as pltpu
from jax.sharding import PartitionSpec as P

MESH = pl.DeviceIdType.MESH
mix_rate = 0.5
COLUMNS = 2
PIECES = 6
EXTRAS = 2


def queues_of(z, length):
    every = list(range(PIECES + EXTRAS))
    late = list(range(PIECES // 2, PIECES))
    early = [c for c in every if c not in late]
    out = {"up": [], "down": [], "side": []}
    if z < length - 1:
        out["up"] += [(z - s, 0, c) for s in range(z + 1) for c in every]
        if z == 0:
            out["up"] += [(0, 1, c) for c in every]
        if z == length - 2:
            out["up"] += [(z, 1, c) for c in late]
    if z > 0:
        out["down"] += [(z + s, 0, c) for s in range(length - z) for c in every]
        if z == length - 1:
            out["down"] += [(z, 1, c) for c in every]
        if z == 1:
            out["down"] += [(z, 1, c) for c in late]
    for b in sorted(range(length), key=lambda b: (abs(b - z), b)):
        pieces = every
        if (z, b) in ((0, 1), (length - 1, length - 2)):
            pieces = early
        if (z, b) in ((1, 0), (length - 2, length - 1)):
            pieces = []
        out["side"] += [(b, 0, c) for c in pieces]
    return out


def order_of(length):
    size = [1.0] * PIECES + [0.1, 0.03]
    queues = [queues_of(z, length) for z in range(length)]
    far = 1e9
    there = [{} for _ in range(length)]
    for z in range(length):
        for c in range(PIECES + EXTRAS):
            there[z][z, 0, c] = 0.0 if c < PIECES else 1.0
    for _ in range(4 * length):
        for z in range(length):
            for name, queue in queues[z].items():
                now = 0.0
                for b, o, c in queue:
                    now = max(now, there[z].get((b, o, c), far)) + size[c]
                    to = {"up": z + 1, "down": z - 1, "side": z}[name]
                    key = (b, 1 - o if name == "side" else o, c)
                    there[to][key] = now
    result = []
    for z in range(length):
        events = []
        for name, queue in queues[z].items():
            key = 0.0
            for at, (b, o, c) in enumerate(queue):
                key = max(key, there[z][b, o, c])
                events.append((key, at, name, b, o, c))
        result.append(sorted(events))
        assert max(e[0] for e in events) < far
    return result


def gather_kernel(
    n_zero, n_model,
    w_q, w_k, w_v, l_q, l_k, l_v, h_q, h_k, h_v, n_a, n_b,
    g_q, g_k, g_v, lows, sums, norms,
    w_vm, h_vm, lt_vm, ps_vm, na_vm, nb_vm, ns_vm,
    send_sem, recv_sem, load_sem, store_sem, nsend_sem, nrecv_sem,
):
    w, low, high, gathered = (w_q, w_k, w_v), (l_q, l_k, l_v), (h_q, h_k, h_v), (g_q, g_k, g_v)
    length = n_zero // COLUMNS
    zero, model = lax.axis_index("zero"), lax.axis_index("model")
    place, column = zero // COLUMNS, zero % COLUMNS
    rows, rank = w_q.shape[0], l_q.shape[0]
    half = rows // 2
    count = n_zero * n_model
    me = zero * n_model + model

    loads = []
    for m in range(3):
        loads.append(pltpu.make_async_copy(w[m], w_vm.at[m], load_sem.at[m]))
        into = lt_vm.at[pl.ds(m * rank, rank)]
        loads.append(pltpu.make_async_copy(low[m], into, load_sem.at[3 + m]))
        loads.append(pltpu.make_async_copy(high[m], h_vm.at[m], load_sem.at[6 + m]))
    loads.append(pltpu.make_async_copy(n_a, na_vm, load_sem.at[9]))
    loads.append(pltpu.make_async_copy(n_b, nb_vm, load_sem.at[10]))
    for load in loads:
        load.start()

    barrier = pltpu.get_barrier_semaphore()

    def greet(k, carry):
        to = lax.rem(me + k, count)
        pl.semaphore_signal(
            barrier, inc=1, device_id=(to // n_model, to % n_model), device_id_type=MESH
        )
        return carry

    lax.fori_loop(1, count, greet, 0)
    pl.semaphore_wait(barrier, count - 1)

    def block_at(b, o):
        return b * COLUMNS + (column if o == 0 else 1 - column)

    def landing(block, c):
        if c < PIECES:
            first = pl.multiple_of(block * rows, rows) + (c % 2) * half
            return gathered[c // 2].at[pl.ds(pl.multiple_of(first, half), half)]
        return (lows, sums)[c - PIECES].at[block]

    lane_of = {"up": 0, "down": 1, "side": 2}

    def copy_of(z, name, at, b, o, c):
        block = block_at(b, o)
        target = {
            "up": (z + 1) * COLUMNS + column,
            "down": (z - 1) * COLUMNS + column,
            "side": z * COLUMNS + 1 - column,
        }[name]
        own = b == z and o == 0
        if own and c < PIECES:
            source = w[c // 2].at[pl.ds((c % 2) * half, half)]
        elif own:
            source = (lt_vm, ps_vm)[c - PIECES]
        else:
            source = landing(block, c)
        return pltpu.make_async_remote_copy(
            src_ref=source,
            dst_ref=landing(block, c),
            send_sem=send_sem.at[lane_of[name], at],
            recv_sem=recv_sem.at[block, c],
            device_id=(target, model),
            device_id_type=MESH,
        )

    def arrival(b, o, c):
        block = block_at(b, o)
        return pltpu.make_async_copy(
            landing(block, c), landing(block, c), recv_sem.at[block, c]
        )

    orders = order_of(length)
    for z in range(length):

        @pl.when(place == z)
        def _(z=z):
            for key, at, name, b, o, c in orders[z]:
                if b == z and o == 0 and c < PIECES:
                    copy_of(z, name, at, b, o, c).start()

    for load in loads:
        load.wait()
    stores = []
    for m in range(3):
        into = gathered[m].at[pl.ds(pl.multiple_of(zero * rows, rows), rows)]
        stores.append(pltpu.make_async_copy(w_vm.at[m], into, store_sem.at[m]))
        stores[-1].start()
    ns_vm[...] = na_vm[...] + nb_vm[...]
    tile = 128
    for m in range(3):

        def add(i, total, m=m):
            at = pl.ds(pl.multiple_of(i * tile, tile), tile)
            mixed = lax.dot_general(
                lt_vm[m * rank : (m + 1) * rank, at],
                h_vm[m],
                (((0,), (0,)), ((), ())),
                preferred_element_type=jnp.float32,
            )
            whole = w_vm[m, at, :].astype(jnp.float32) + mix_rate * mixed
            return total + jnp.sum(
                jnp.abs(whole).reshape(tile // 8, 8, whole.shape[1]), axis=0
            )

        total = lax.fori_loop(
            0, rows // tile, add, jnp.zeros((8, w_vm.shape[2]), jnp.float32)
        )
        ps_vm[m : m + 1, :] = jnp.sum(total, axis=0, keepdims=True)

    def norm_copy(k):
        to = lax.rem(me + k, count)
        return pltpu.make_async_remote_copy(
            src_ref=ns_vm,
            dst_ref=norms.at[me],
            send_sem=nsend_sem.at[k],
            recv_sem=nrecv_sem.at[me],
            device_id=(to // n_model, to % n_model),
            device_id_type=MESH,
        )

    own = [
        pltpu.make_async_copy(lt_vm, lows.at[zero], store_sem.at[3]),
        pltpu.make_async_copy(ps_vm, sums.at[zero], store_sem.at[4]),
        pltpu.make_async_copy(ns_vm, norms.at[me], store_sem.at[5]),
    ]

    for z in range(length):

        @pl.when(place == z)
        def _(z=z):
            seen = set()
            for key, at, name, b, o, c in orders[z]:
                mine = b == z and o == 0
                if mine and c < PIECES:
                    continue
                if not mine and (b, o, c) not in seen:
                    seen.add((b, o, c))
                    arrival(b, o, c).wait()
                copy_of(z, name, at, b, o, c).start()
            for b in range(length):
                for o in range(2):
                    for c in range(PIECES + EXTRAS):
                        if (b, o) != (z, 0) and (b, o, c) not in seen:
                            arrival(b, o, c).wait()
            for key, at, name, b, o, c in orders[z]:
                copy_of(z, name, at, b, o, c).wait_send()

    for copy in own:
        copy.start()

    def send_norm(k, carry):
        norm_copy(k).start()
        return carry

    lax.fori_loop(1, count, send_norm, 0)
    for copy in stores + own:
        copy.wait()

    def end_norm(k, carry):
        norm_copy(k).wait_send()
        origin = lax.rem(me + k, count)
        pltpu.make_async_copy(norms.at[origin], norms.at[origin], nrecv_sem.at[origin]).wait()
        return carry

    lax.fori_loop(1, count, end_norm, 0)


def finish_kernel(d_model, g_q, g_k, g_v, lt, h_q, h_k, h_v, sums, s_q, s_k, s_v, f_q, f_k, f_v):
    rank = h_q.shape[0]
    for m, (g, h, s, f) in enumerate(
        ((g_q, h_q, s_q, f_q), (g_k, h_k, s_k, f_k), (g_v, h_v, s_v, f_v))
    ):
        factor = jnp.sum(sums[:, m, :], axis=0, keepdims=True) / d_model
        f[...] = factor
        scale = 1.0 / factor
        mixed = lax.dot_general(
            lt[0, m * rank : (m + 1) * rank, :],
            h[...],
            (((0,), (0,)), ((), ())),
            preferred_element_type=jnp.float32,
        )
        whole = g[...].astype(jnp.float32) + mix_rate * mixed
        s[...] = (whole * scale).astype(s.dtype)


def on_lines(n_zero, n_model, w_q, l_q, h_q, w_k, l_k, h_k, w_v, l_v, h_v, n_a, n_b):
    rows, width = w_q.shape
    rank = l_q.shape[1]
    d_model = rows * n_zero
    count = n_zero * n_model
    share = n_a.shape[0]
    sends = (n_zero // COLUMNS) * (PIECES + EXTRAS) + PIECES
    f32, bf16 = jnp.float32, jnp.bfloat16
    shape = jax.ShapeDtypeStruct
    anywhere = pl.BlockSpec(memory_space=pl.ANY)
    dma = pltpu.SemaphoreType.DMA
    g_q, g_k, g_v, lows, sums, norms = pl.pallas_call(
        functools.partial(gather_kernel, n_zero, n_model),
        out_shape=(
            shape((d_model, width), bf16),
            shape((d_model, width), bf16),
            shape((d_model, width), bf16),
            shape((n_zero, 3 * rank, rows), bf16),
            shape((n_zero, 3, width), f32),
            shape((count, 1, share), f32),
        ),
        in_specs=[anywhere] * 11,
        out_specs=(anywhere,) * 6,
        scratch_shapes=[
            pltpu.VMEM((3, rows, width), bf16),
            pltpu.VMEM((3, rank, width), bf16),
            pltpu.VMEM((3 * rank, rows), bf16),
            pltpu.VMEM((3, width), f32),
            pltpu.VMEM((1, share), f32),
            pltpu.VMEM((1, share), f32),
            pltpu.VMEM((1, share), f32),
            dma((3, sends)),
            dma((n_zero, PIECES + EXTRAS)),
            dma((11,)),
            dma((6,)),
            dma((count,)),
            dma((count,)),
        ],
        compiler_params=pltpu.CompilerParams(collective_id=0, has_side_effects=True),
    )(w_q, w_k, w_v, l_q.T, l_k.T, l_v.T, h_q, h_k, h_v, n_a.reshape(1, share), n_b.reshape(1, share))

    tile = rows // 2
    tall = pl.BlockSpec((tile, width), lambda i: (i, 0))
    wide = pl.BlockSpec((rank, width), lambda i: (0, 0))
    line = pl.BlockSpec((1, width), lambda i: (0, 0))
    s_q, s_k, s_v, f_q, f_k, f_v = pl.pallas_call(
        functools.partial(finish_kernel, d_model),
        grid=(d_model // tile,),
        out_shape=(shape((d_model, width), bf16),) * 3 + (shape((1, width), f32),) * 3,
        in_specs=[tall] * 3
        + [pl.BlockSpec((1, 3 * rank, tile), lambda i: (i // 2, 0, i % 2))]
        + [wide] * 3
        + [pl.BlockSpec((n_zero, 3, width), lambda i: (0, 0, 0))],
        out_specs=(tall,) * 3 + (line,) * 3,
        compiler_params=pltpu.CompilerParams(dimension_semantics=("arbitrary",)),
    )(g_q, g_k, g_v, lows, h_q, h_k, h_v, sums)
    norm = norms.astype(bf16).reshape(count * share)
    return (
        s_q, s_k, s_v, f_q.reshape(width), f_k.reshape(width), f_v.reshape(width), norm,
    )


def plain(n_zero, n_model, w_q, l_q, h_q, w_k, l_k, h_k, w_v, l_v, h_v, n_a, n_b):
    d_model = w_q.shape[0] * n_zero
    wholes = [
        w.astype(jnp.float32) + mix_rate * jnp.dot(l, h, preferred_element_type=jnp.float32)
        for w, l, h in ((w_q, l_q, h_q), (w_k, l_k, h_k), (w_v, l_v, h_v))
    ]
    totals = lax.psum([jnp.sum(jnp.abs(whole), axis=0) for whole in wholes], "zero")
    factors = [total / d_model for total in totals]
    serving = [
        lax.all_gather((whole / factor).astype(jnp.bfloat16), "zero", axis=0, tiled=True)
        for whole, factor in zip(wholes, factors)
    ]
    norm = lax.all_gather(
        (n_a + n_b).astype(jnp.bfloat16), ("zero", "model"), axis=0, tiled=True
    )
    return (*serving, *factors, norm)


def solution(mesh):
    n_zero, n_model = mesh.shape["zero"], mesh.shape["model"]
    lines = n_zero == 2 * n_model
    tall, low, wide = P("zero", "model"), P("zero", None), P(None, "model")
    return jax.shard_map(
        functools.partial(on_lines if lines else plain, n_zero, n_model),
        mesh=mesh,
        in_specs=(tall, low, wide) * 3 + (P(("zero", "model")),) * 2,
        out_specs=(wide,) * 3 + (P("model"),) * 3 + (P(),),
        check_vma=False,
    )
```

```python
import functools

import jax
import jax.numpy as jnp
from jax import lax
from jax.experimental import pallas as pl
from jax.experimental.pallas import tpu as pltpu
from jax.sharding import PartitionSpec as P

MESH = pl.DeviceIdType.MESH
mix_rate = 0.5
VMEM_MOST = 67_043_328
SPARE = 65_536
COLUMNS = 2
PIECES = 6
WRITES = 4
FIRST = 2


def queues_of(z, length):
    every = [PIECES] + list(range(PIECES))
    late = list(range(PIECES // 2, PIECES))
    early = [c for c in every if c not in late]
    out = {"up": [], "down": [], "side": []}
    if z < length - 1:
        out["up"] += [(z - s, 0, c) for s in range(z + 1) for c in every]
        if z == 0:
            out["up"] += [(0, 1, c) for c in every]
        if z == length - 2:
            out["up"] += [(z, 1, c) for c in late]
    if z > 0:
        out["down"] += [(z + s, 0, c) for s in range(length - z) for c in every]
        if z == length - 1:
            out["down"] += [(z, 1, c) for c in every]
        if z == 1:
            out["down"] += [(z, 1, c) for c in late]
    for b in sorted(range(length), key=lambda b: (abs(b - z), b)):
        pieces = every
        if (z, b) in ((0, 1), (length - 1, length - 2)):
            pieces = early
        if (z, b) in ((1, 0), (length - 2, length - 1)):
            pieces = []
        out["side"] += [(b, 0, c) for c in pieces]
    return out


def order_of(length):
    size = [1.0] * PIECES + [0.1]
    queues = [queues_of(z, length) for z in range(length)]
    far = 1e9
    there = [{} for _ in range(length)]
    for z in range(length):
        for c in range(PIECES + 1):
            there[z][z, 0, c] = 0.0
    for _ in range(4 * length):
        for z in range(length):
            for name, queue in queues[z].items():
                now = 0.0
                for b, o, c in queue:
                    now = max(now, there[z].get((b, o, c), far)) + size[c]
                    to = {"up": z + 1, "down": z - 1, "side": z}[name]
                    key = (b, 1 - o if name == "side" else o, c)
                    there[to][key] = now
    result = []
    for z in range(length):
        events = []
        for name, queue in queues[z].items():
            key = 0.0
            for at, (b, o, c) in enumerate(queue):
                key = max(key, there[z][b, o, c])
                events.append((key, at, name, b, o, c))
        assert max(e[0] for e in events) < far
        result.append((sorted(events), there[z]))
    return result


def gather_kernel(
    n_zero, n_model,
    w_q, w_k, w_v, l_q, l_k, l_v, h_q, h_k, h_v, n_a, n_b,
    s_q, s_k, s_v, factors, norms, g_q, g_k, g_v,
    w_vm, h_vm, stage, lows, sums, scales, na_vm, nb_vm, ns_vm,
    send_sem, recv_sem, load_sem, store_sem, stage_sem, ssend_sem, srecv_sem, nsend_sem, nrecv_sem,
):
    w, low, high, gathered = (w_q, w_k, w_v), (l_q, l_k, l_v), (h_q, h_k, h_v), (g_q, g_k, g_v)
    served = (s_q, s_k, s_v)
    length = n_zero // COLUMNS
    zero, model = lax.axis_index("zero"), lax.axis_index("model")
    place, column = zero // COLUMNS, zero % COLUMNS
    rows, rank = w_q.shape[0], l_q.shape[0]
    half = rows // 2
    count = n_zero * n_model
    me = zero * n_model + model

    loads = []
    for m in range(3):
        into = lows.at[zero, pl.ds(m * rank, rank)]
        loads.append(pltpu.make_async_copy(low[m], into, load_sem.at[m]))
    for m in range(3):
        loads.append(pltpu.make_async_copy(w[m], w_vm.at[m], load_sem.at[3 + m]))
        loads.append(pltpu.make_async_copy(high[m], h_vm.at[m], load_sem.at[6 + m]))
    loads.append(pltpu.make_async_copy(n_a, na_vm, load_sem.at[9]))
    loads.append(pltpu.make_async_copy(n_b, nb_vm, load_sem.at[10]))
    for load in loads:
        load.start()

    barrier = pltpu.get_barrier_semaphore()

    def greet(k, carry):
        to = lax.rem(me + k, count)
        pl.semaphore_signal(
            barrier, inc=1, device_id=(to // n_model, to % n_model), device_id_type=MESH
        )
        return carry

    lax.fori_loop(1, count, greet, 0)
    pl.semaphore_wait(barrier, count - 1)
    for load in loads:
        load.wait()

    def block_at(b, o):
        return b * COLUMNS + (column if o == 0 else 1 - column)

    def landing(block, c):
        if c < PIECES:
            first = pl.multiple_of(block * rows, rows) + (c % 2) * half
            return gathered[c // 2].at[pl.ds(pl.multiple_of(first, half), half)]
        return lows.at[block]

    lane_of = {"up": 0, "down": 1, "side": 2}

    def copy_of(z, name, at, b, o, c):
        block = block_at(b, o)
        target = {
            "up": (z + 1) * COLUMNS + column,
            "down": (z - 1) * COLUMNS + column,
            "side": z * COLUMNS + 1 - column,
        }[name]
        source = landing(block, c)
        if b == z and o == 0 and c < PIECES:
            source = w[c // 2].at[pl.ds((c % 2) * half, half)]
        return pltpu.make_async_remote_copy(
            src_ref=source,
            dst_ref=landing(block, c),
            send_sem=send_sem.at[lane_of[name], at],
            recv_sem=recv_sem.at[block, c],
            device_id=(target, model),
            device_id_type=MESH,
        )

    def arrive(b, o, c):
        block = block_at(b, o)
        pltpu.make_async_copy(
            landing(block, c), landing(block, c), recv_sem.at[block, c]
        ).wait()

    def send_own(pieces):
        for z in range(length):

            @pl.when(place == z)
            def _(z=z):
                for key, at, name, b, o, c in orders[z][0]:
                    if b == z and o == 0 and c in pieces:
                        copy_of(z, name, at, b, o, c).start()

    orders = order_of(length)
    send_own((PIECES, *range(FIRST)))

    def whole_of(m, block, source, at):
        mixed = lax.dot_general(
            lows[block, pl.ds(m * rank, rank), at],
            h_vm[m],
            (((0,), (0,)), ((), ())),
            preferred_element_type=jnp.float32,
        )
        return source[at, :].astype(jnp.float32) + mix_rate * mixed

    tile = 128
    ns_vm[...] = na_vm[...] + nb_vm[...]
    for m in range(3):

        def add(i, total, m=m):
            at = pl.ds(pl.multiple_of(i * tile, tile), tile)
            whole = whole_of(m, zero, w_vm.at[m], at)
            return total + jnp.sum(
                jnp.abs(whole).reshape(tile // 8, 8, whole.shape[1]), axis=0
            )

        total = lax.fori_loop(
            0, rows // tile, add, jnp.zeros((8, w_vm.shape[2]), jnp.float32)
        )
        sums[zero, m : m + 1, :] = jnp.sum(total, axis=0, keepdims=True)

    def sum_copy(k):
        to = lax.rem(zero + k, n_zero)
        return pltpu.make_async_remote_copy(
            src_ref=sums.at[zero],
            dst_ref=sums.at[zero],
            send_sem=ssend_sem.at[k],
            recv_sem=srecv_sem.at[zero],
            device_id=(to, model),
            device_id_type=MESH,
        )

    def norm_copy(k):
        to = lax.rem(me + k, count)
        return pltpu.make_async_remote_copy(
            src_ref=ns_vm,
            dst_ref=norms.at[me],
            send_sem=nsend_sem.at[k],
            recv_sem=nrecv_sem.at[me],
            device_id=(to // n_model, to % n_model),
            device_id_type=MESH,
        )

    for k in range(1, n_zero):
        sum_copy(k).start()
    send_own(tuple(range(FIRST, PIECES)))

    def send_norm(k, carry):
        norm_copy(k).start()
        return carry

    lax.fori_loop(1, count, send_norm, 0)
    own_norm = pltpu.make_async_copy(ns_vm, norms.at[me], store_sem)
    own_norm.start()

    for k in range(1, n_zero):
        origin = lax.rem(zero + k, n_zero)
        pltpu.make_async_copy(sums.at[origin], sums.at[origin], srecv_sem.at[origin]).wait()
        sum_copy(k).wait_send()
    factor = jnp.sum(sums[...], axis=0) / (rows * n_zero)
    factors[...] = factor
    scales[...] = 1.0 / factor

    def finish(m, block, source):
        base = pl.multiple_of(block * rows, rows)

        def step(i, carry):
            first = pl.multiple_of(i * tile, tile)
            whole = whole_of(m, block, source, pl.ds(first, tile))
            to = pl.ds(pl.multiple_of(base + first, tile), tile)
            served[m][to, :] = (whole * scales[m : m + 1, :]).astype(s_q.dtype)
            return carry

        lax.fori_loop(0, rows // tile, step, 0)

    for m in range(3):
        finish(m, zero, w_vm.at[m])

    for z in range(length):

        @pl.when(place == z)
        def _(z=z):
            events, there = orders[z]
            items = [(key, 0, at, name, b, o, c) for key, at, name, b, o, c in events]
            for b in range(length):
                for o in range(COLUMNS):
                    if (b, o) != (z, 0):
                        for m in range(3):
                            when = max(there[b, o, c] for c in (2 * m, 2 * m + 1, PIECES))
                            items.append((when, 1, m, "", b, o, 0))
            seen = set()

            def need(b, o, c):
                if (b, o) != (z, 0) and (b, o, c) not in seen:
                    seen.add((b, o, c))
                    arrive(b, o, c)

            for _, kind, at, name, b, o, c in sorted(items):
                if kind == 0:
                    if (b, o) != (z, 0):
                        need(b, o, c)
                        copy_of(z, name, at, b, o, c).start()
                    continue
                for piece in (2 * at, 2 * at + 1, PIECES):
                    need(b, o, piece)
                block = block_at(b, o)
                raw = gathered[at].at[pl.ds(pl.multiple_of(block * rows, rows), rows)]
                load = pltpu.make_async_copy(raw, stage, stage_sem)
                load.start()
                load.wait()
                finish(at, block, stage)
            for key, at, name, b, o, c in events:
                copy_of(z, name, at, b, o, c).wait_send()

    own_norm.wait()

    def end_norm(k, carry):
        norm_copy(k).wait_send()
        origin = lax.rem(me + k, count)
        pltpu.make_async_copy(norms.at[origin], norms.at[origin], nrecv_sem.at[origin]).wait()
        return carry

    lax.fori_loop(1, count, end_norm, 0)


def write_kernel(s_q, s_k, s_v, factors, o_q, o_k, o_v, f_q, f_k, f_v, sem):
    rows = s_q.shape[0] // WRITES
    copies = []
    for m, (s, o) in enumerate(((s_q, o_q), (s_k, o_k), (s_v, o_v))):
        for i in range(WRITES):
            part = pl.ds(i * rows, rows)
            copies.append(pltpu.make_async_copy(s.at[part], o.at[part], sem.at[m * WRITES + i]))
            copies[-1].start()
    for m, f in enumerate((f_q, f_k, f_v)):
        f[...] = factors[m : m + 1, :]
    for copy in copies:
        copy.wait()


def on_lines(n_zero, n_model, w_q, l_q, h_q, w_k, l_k, h_k, w_v, l_v, h_v, n_a, n_b):
    rows, width = w_q.shape
    rank = l_q.shape[1]
    d_model = rows * n_zero
    count = n_zero * n_model
    share = n_a.shape[0]
    sends = (n_zero // COLUMNS) * (PIECES + 1) + PIECES
    f32, bf16 = jnp.float32, jnp.bfloat16
    shape = jax.ShapeDtypeStruct
    anywhere = pl.BlockSpec(memory_space=pl.ANY)
    inside = pl.BlockSpec(memory_space=pltpu.VMEM)
    dma = pltpu.SemaphoreType.DMA
    tall = (d_model, width)
    s_q, s_k, s_v, factors, norms, _, _, _ = pl.pallas_call(
        functools.partial(gather_kernel, n_zero, n_model),
        out_shape=(pltpu.VMEM(tall, bf16),) * 3
        + (shape((3, width), f32), shape((count, 1, share), f32))
        + (shape(tall, bf16),) * 3,
        in_specs=[anywhere] * 11,
        out_specs=(inside,) * 4 + (anywhere,) * 4,
        scratch_shapes=[
            pltpu.VMEM((3, rows, width), bf16),
            pltpu.VMEM((3, rank, width), bf16),
            pltpu.VMEM((rows, width), bf16),
            pltpu.VMEM((n_zero, 3 * rank, rows), bf16),
            pltpu.VMEM((n_zero, 3, width), f32),
            pltpu.VMEM((3, width), f32),
            pltpu.VMEM((1, share), f32),
            pltpu.VMEM((1, share), f32),
            pltpu.VMEM((1, share), f32),
            dma((3, sends)),
            dma((n_zero, PIECES + 1)),
            dma((11,)),
            dma,
            dma,
            dma((n_zero,)),
            dma((n_zero,)),
            dma((count,)),
            dma((count,)),
        ],
        compiler_params=pltpu.CompilerParams(
            collective_id=0, has_side_effects=True, vmem_limit_bytes=VMEM_MOST - 3 * d_model * width * 2 - SPARE
        ),
    )(w_q, w_k, w_v, l_q.T, l_k.T, l_v.T, h_q, h_k, h_v, n_a.reshape(1, share), n_b.reshape(1, share))
    *served, f_q, f_k, f_v = pl.pallas_call(
        write_kernel,
        out_shape=(shape(tall, bf16),) * 3 + (shape((1, width), f32),) * 3,
        in_specs=[anywhere] * 3 + [inside],
        out_specs=(anywhere,) * 3 + (inside,) * 3,
        scratch_shapes=[dma((3 * WRITES,))],
        compiler_params=pltpu.CompilerParams(
            vmem_limit_bytes=4 * 1024 * 1024
        ),
    )(s_q, s_k, s_v, factors)
    norm = norms.astype(bf16).reshape(count * share)
    return (*served, f_q.reshape(width), f_k.reshape(width), f_v.reshape(width), norm)


def plain(n_zero, n_model, w_q, l_q, h_q, w_k, l_k, h_k, w_v, l_v, h_v, n_a, n_b):
    d_model = w_q.shape[0] * n_zero
    wholes = [
        w.astype(jnp.float32) + mix_rate * jnp.dot(l, h, preferred_element_type=jnp.float32)
        for w, l, h in ((w_q, l_q, h_q), (w_k, l_k, h_k), (w_v, l_v, h_v))
    ]
    totals = lax.psum([jnp.sum(jnp.abs(whole), axis=0) for whole in wholes], "zero")
    factors = [total / d_model for total in totals]
    serving = [
        lax.all_gather((whole / factor).astype(jnp.bfloat16), "zero", axis=0, tiled=True)
        for whole, factor in zip(wholes, factors)
    ]
    norm = lax.all_gather(
        (n_a + n_b).astype(jnp.bfloat16), ("zero", "model"), axis=0, tiled=True
    )
    return (*serving, *factors, norm)


def solution(mesh):
    n_zero, n_model = mesh.shape["zero"], mesh.shape["model"]
    lines = n_zero == 2 * n_model
    tall, low, wide = P("zero", "model"), P("zero", None), P(None, "model")
    return jax.shard_map(
        functools.partial(on_lines if lines else plain, n_zero, n_model),
        mesh=mesh,
        in_specs=(tall, low, wide) * 3 + (P(("zero", "model")),) * 2,
        out_specs=(wide,) * 3 + (P("model"),) * 3 + (P(),),
        check_vma=False,
    )
```
